256 devices in a mesh: fsdp: 16 (over y, x), width: 16 (over z, core).
Axes of the slice: x: 4, y: 4, z: 8, core: 2. Of those that a mesh axis runs over, the one named last changes fastest.
Arguments:
- train_gate: float32 [4096, 11008], P('fsdp', 'width'), may hold values from -0.125 to 0.125
- drift_gate: float32 [4096, 11008], P('fsdp', 'width'), may hold values from -0.09375 to 0.09375
- spread_gate: float32 [4096, 11008], P('fsdp', 'width'), may hold values from -0.09375 to 0.09375
- train_up: float32 [4096, 11008], P('fsdp', 'width'), may hold values from -0.125 to 0.125
- drift_up: float32 [4096, 11008], P('fsdp', 'width'), may hold values from -0.09375 to 0.09375
- spread_up: float32 [4096, 11008], P('fsdp', 'width'), may hold values from -0.09375 to 0.09375
- norm_train: float32 [4096], P(('fsdp', 'width')), may hold values from 0.25 to 1.75
- norm_step: float32 [4096], P(('fsdp', 'width')), may hold values from -0.3 to 0.3
Outputs:
- serving_gate: bfloat16 [4096, 11008], P(None, 'width')
- serving_up: bfloat16 [4096, 11008], P(None, 'width')
- scale_gate: float32 [11008], P('width')
- scale_up: float32 [11008], P('width')
- serve_norm: bfloat16 [4096], replicated
- whole_gate: float32 [4096, 11008], P('fsdp', 'width')
- whole_up: float32 [4096, 11008], P('fsdp', 'width')
The draws below stay inside these ranges and needn't reach their ends.
All inputs are finite; a program needn't handle non-finite values.
Results may differ from the reference program's by a relative error of at most 0.0004.
Values may be sent and summed in bfloat16 or wider, within the bound.
A program may use at most 128 MiB of HBM per device.

```python
import jax
import jax.numpy as jnp
from jax import lax

D_MODEL = 4096
D_INNER = 11008


def strengthened(entries, key, source, target, shards_of, factor):
    def block_of(axis_at):
        return (jnp.arange(entries.shape[axis_at]) // (entries.shape[axis_at] // shards_of)).reshape((-1,) + (1,) * (entries.ndim - 1 - axis_at))

    one_side = jax.random.permutation(key, shards_of)[block_of(target)]
    other_side = (block_of(target) + shards_of // 2) % shards_of
    return jnp.where((block_of(source) == one_side) | (block_of(source) == other_side), factor * entries, entries)


def level_of(own_key, dims, split, smallest, largest):
    loudness = 1.0
    for position, parts in split:
        draws = jax.random.uniform(jax.random.fold_in(jax.random.fold_in(own_key, 6), position), (parts,), jnp.float32, smallest / len(split), largest / len(split))
        loudness = loudness * jnp.repeat(jnp.exp(draws), dims[position] // parts).reshape((-1,) + (1,) * (len(dims) - 1 - position))
    return loudness


def gaussian(own_key, dims, width, reach, cuts=(), held_as=jnp.bfloat16):
    array = width * jax.random.normal(own_key, dims, jnp.float32)
    if cuts:
        array = array * level_of(own_key, dims, cuts, -0.22, 0.18)
    return jnp.clip(array, -reach, reach).astype(held_as)


def bell_draw_with(own_key, shape, spread, reach, split, heavy, dtype=jnp.bfloat16):
    values = spread * jax.random.normal(own_key, shape, jnp.float32)
    if split:
        values = values * level_of(own_key, shape, split, -0.22, 0.18)
    return jnp.clip(strengthened(values, jax.random.fold_in(own_key, 3), *heavy), -reach, reach).astype(dtype)


def setup_inputs(seed: int = 0) -> dict:
    seeds = jax.random.split(jax.random.key(seed), 9)
    return {
        "train_gate": bell_draw_with(seeds[0], (D_MODEL, D_INNER), D_MODEL ** -0.5, 0.125, ((0, 16), (1, 16)), (0, 1, 16, 2.0), jnp.float32),
        "drift_gate": gaussian(seeds[1], (D_MODEL, D_INNER), D_MODEL ** -0.5, 0.09375, ((0, 16), (1, 16)), jnp.float32),
        "spread_gate": gaussian(seeds[2], (D_MODEL, D_INNER), D_MODEL ** -0.5, 0.09375, ((0, 16), (1, 16)), jnp.float32),
        "train_up": bell_draw_with(seeds[3], (D_MODEL, D_INNER), D_MODEL ** -0.5, 0.125, ((0, 16), (1, 16)), (0, 1, 16, 2.0), jnp.float32),
        "drift_up": gaussian(seeds[4], (D_MODEL, D_INNER), D_MODEL ** -0.5, 0.09375, ((0, 16), (1, 16)), jnp.float32),
        "spread_up": gaussian(seeds[5], (D_MODEL, D_INNER), D_MODEL ** -0.5, 0.09375, ((0, 16), (1, 16)), jnp.float32),
        "norm_train": jnp.clip(1.0 + 0.15 * jax.random.normal(seeds[6], (D_MODEL,), jnp.float32), 0.25, 1.75),
        "norm_step": jnp.clip(jax.random.uniform(seeds[7], (D_MODEL,), jnp.float32, -0.3, 0.3) * level_of(seeds[7], (D_MODEL,), ((0, 256),), -0.4, 0.0), -0.3, 0.3),
    }


learn_rate = 0.3
hold_rate = 0.9

def reference(train_gate, drift_gate, spread_gate, train_up, drift_up, spread_up, norm_train, norm_step):
    hold_gate = hold_rate * drift_gate + spread_gate
    whole_gate = train_gate - learn_rate * hold_gate
    hold_up = hold_rate * drift_up + spread_up
    whole_up = train_up - learn_rate * hold_up
    scale_gate = jnp.sqrt(lax.optimization_barrier(jnp.sum(whole_gate * whole_gate, axis=0)))
    serving_gate = (whole_gate / scale_gate).astype(jnp.bfloat16)
    scale_up = jnp.sqrt(lax.optimization_barrier(jnp.sum(whole_up * whole_up, axis=0)))
    serving_up = (whole_up / scale_up).astype(jnp.bfloat16)
    serve_norm = (norm_train + norm_step).astype(jnp.bfloat16)
    return (serving_gate, serving_up, scale_gate, scale_up, serve_norm, whole_gate, whole_up)
```

```python
import functools

import jax
import jax.numpy as jnp
from jax import lax
from jax.experimental import pallas as pl
from jax.experimental.pallas import tpu as pltpu
from jax.sharding import Mesh
from jax.sharding import PartitionSpec as P

FSDP = ("fsdp_0", "fsdp_1")
FSDP_WIDTH = ("fsdp_0", "fsdp_1", "width")
RING = 4
LANES = 128
NORM_ROW = 14

learn_rate = 0.3
hold_rate = 0.9


def chunks(columns):
    return [(at, min(LANES, columns - at)) for at in range(0, columns, LANES)]


def kernel(n_width, tg, dg, sg, tu, du, su, norm,
           og, ou, scale_g, scale_u, serve, wg, wu,
           held, sums, parts, ordered,
           in_sems, sum_send, sum_recv, part_send, part_recv, send_sems, recv_sems):
    y, x, w = lax.axis_index("fsdp_0"), lax.axis_index("fsdp_1"), lax.axis_index("width")
    me = y * RING + x
    columns, rows = wg.shape

    def at(yy, xx, ww):
        return {"device_id": (yy, xx, ww), "device_id_type": pl.DeviceIdType.MESH}

    loads = [pltpu.make_async_copy(ref, held.at[i], in_sems.at[i])
             for i, ref in enumerate((tg, dg, sg, tu, du, su))]
    for load in loads:
        load.start()

    plane = sorted(((dy, dx) for dy in range(RING) for dx in range(RING) if dy or dx),
                   key=lambda d: -(min(d[0], RING - d[0]) + min(d[1], RING - d[1])))
    mates = [((y + dy) % RING, (x + dx) % RING, w) for dy, dx in plane]
    stack = [(y, x, (w + dw) % n_width) for dw in range(1, n_width)]

    barrier = pltpu.get_barrier_semaphore()
    for peer in mates + stack:
        pl.semaphore_signal(barrier, 1, **at(*peer))

    sums[me] = jnp.zeros((16, LANES), jnp.float32)
    sums[me, NORM_ROW:NORM_ROW + 1, :] = norm[...]
    for a, whole in enumerate((wg, wu)):
        for load in loads[3 * a:3 * a + 3]:
            load.wait()
        for k, (start, size) in enumerate(chunks(columns)):
            part = pl.ds(start, size)
            hold = hold_rate * held[3 * a + 1, part, :] + held[3 * a + 2, part, :]
            new = held[3 * a, part, :] - learn_rate * hold
            whole[part, :] = new
            square = new * new
            folded = square[:, :LANES]
            for j in range(LANES, rows, LANES):
                folded = folded + square[:, j:j + LANES]
            if size < LANES:
                folded = jnp.concatenate([folded, jnp.zeros((LANES - size, LANES), jnp.float32)], axis=0)
            sums[me, 8 * a + k:8 * a + k + 1, :] = jnp.sum(folded.T, axis=0, keepdims=True)

    pl.semaphore_wait(barrier, len(mates) + len(stack))

    sent = []
    for i, peer in enumerate(mates):
        copy = pltpu.make_async_remote_copy(sums.at[me], sums.at[me], sum_send.at[i], sum_recv.at[i], **at(*peer))
        copy.start()
        sent.append(copy)
    for i, (dy, dx) in enumerate(plane):
        source = ((y + RING - dy) % RING) * RING + (x + RING - dx) % RING
        pltpu.make_async_remote_copy(sums.at[source], sums.at[source], sum_send.at[i], sum_recv.at[i],
                                     **at(*mates[i])).wait_recv()
    total = sums[0]
    for i in range(1, RING * RING):
        total = total + sums[i]
    scale = jnp.sqrt(total)
    inverse = jnp.concatenate([1.0 / scale, jnp.zeros((LANES - 16, LANES), jnp.float32)], axis=0).T
    own = pl.ds(pl.multiple_of(me * rows, LANES), rows)
    for a, (whole, out) in enumerate(((wg, og), (wu, ou))):
        for k, (start, size) in enumerate(chunks(columns)):
            part = pl.ds(start, size)
            factor = inverse[:size, 8 * a + k:8 * a + k + 1]
            out[part, own] = (whole[part, :] * factor).astype(jnp.bfloat16)
    scale_g[...] = scale[:8]
    scale_u[...] = scale[8:]
    for i in range(RING * RING):
        parts[w, i:i + 1, :] = sums[i, NORM_ROW:NORM_ROW + 1, :]

    half = columns // 2 // 8 * 8
    halves = {1: pl.ds(0, half), -1: pl.ds(half, columns - half)}
    full = pl.ds(0, columns)
    outs = (og, ou)
    keys = {}

    def block(a, p, q):
        p, q = (p + RING) % RING, (q + RING) % RING
        index = q * RING + p if a == 0 else p * RING + q
        return pl.ds(pl.multiple_of(index * rows, LANES), rows)

    def peer(a, phase, d):
        along_x = (a == 0) == (phase == 1)
        if along_x:
            return at(y, (x + d + RING) % RING, w)
        return at((y + d + RING) % RING, x, w)

    def copy_of(key, a, phase, d, part, cols):
        index = keys.setdefault(key, len(keys))
        ref = outs[a].at[part, cols]
        return pltpu.make_async_remote_copy(ref, ref, send_sems.at[index], recv_sems.at[index], **peer(a, phase, d))

    def send(key, a, phase, d, part, cols):
        copy = copy_of(key, a, phase, d, part, cols)
        copy.start()
        sent.append(copy)

    def receive(key, a, phase, d, part, cols):
        copy_of(key, a, phase, d, part, cols).wait_recv()

    spots = ((x, y), (y, x))
    both = [(a, d) for a in range(2) for d in (1, -1)]
    for a, d in both:
        p, q = spots[a]
        send(("first", a, d), a, 1, d, full, block(a, p, q))
    for a, d in both:
        p, q = spots[a]
        send(("second", a, 0, d), a, 2, d, full, block(a, p, q))
    for i, mate in enumerate(stack):
        copy = pltpu.make_async_remote_copy(parts.at[w], parts.at[w], part_send.at[i], part_recv.at[i], **at(*mate))
        copy.start()
        sent.append(copy)
    for a, d in both:
        p, q = spots[a]
        receive(("first", a, d), a, 1, d, full, block(a, p - d, q))
        send(("pass", a, d), a, 1, d, halves[d], block(a, p - d, q))
    for a, e in both:
        p, q = spots[a]
        for d in (1, -1):
            send(("second", a, e, d), a, 2, d, full, block(a, p - e, q))
    for a, e in both:
        p, q = spots[a]
        receive(("pass", a, e), a, 1, e, halves[e], block(a, p - 2 * e, q))
        for d in (1, -1):
            send(("second", a, 2 * e, d), a, 2, d, halves[e], block(a, p + 2, q))
    for e in (0, 1, -1):
        for a, d in both:
            p, q = spots[a]
            receive(("second", a, e, d), a, 2, d, full, block(a, p - e, q - d))
            send(("end", a, e, d), a, 2, d, halves[d], block(a, p - e, q - d))
    for a, d in both:
        p, q = spots[a]
        receive(("second", a, 2 * d, d), a, 2, d, halves[d], block(a, p + 2, q - d))
        send(("end", a, 2, d), a, 2, d, halves[d], block(a, p + 2, q - d))

    for i, (_, _, target) in enumerate(stack):
        source = (w + n_width - (i + 1)) % n_width
        pltpu.make_async_remote_copy(parts.at[source], parts.at[source], part_send.at[i], part_recv.at[i],
                                     **at(*stack[i])).wait_recv()
    strips = ordered.shape[0] // 16
    for b in range(strips):
        group = [parts[i] for i in range(b * n_width // strips, (b + 1) * n_width // strips)]
        ordered[pl.ds(b, 16, stride=strips), :] = functools.reduce(jnp.add, group)
    serve[...] = ordered[...].astype(jnp.bfloat16)

    for a, d in both:
        p, q = spots[a]
        receive(("second", a, -2 * d, d), a, 2, d, halves[-d], block(a, p + 2, q - d))
    for e in (0, 1, -1, 2):
        for a, d in both:
            p, q = spots[a]
            receive(("end", a, e, d), a, 2, d, halves[d], block(a, p - e, q - 2 * d))
    for copy in sent:
        copy.wait_send()


def shards(n_width, train_gate, drift_gate, spread_gate, train_up, drift_up, spread_up, norm_train, norm_step):
    rows, columns = train_gate.shape
    length = norm_train.shape[0]
    strips = n_width * length // LANES
    slot = lax.axis_index("width") * length % LANES // length
    lane = lax.broadcasted_iota(jnp.int32, (1, LANES), 1) // length
    norm = jnp.tile(norm_train + norm_step, LANES // length).reshape(1, LANES)
    norm = jnp.where(lane == slot, norm, 0.0)
    n_copies = 2 * 22
    VMEM, DMA = pltpu.VMEM, pltpu.SemaphoreType.DMA
    space = pl.BlockSpec(memory_space=pltpu.VMEM)
    og, ou, scale_g, scale_u, serve, wg, wu = pl.pallas_call(
        functools.partial(kernel, n_width),
        out_shape=[
            VMEM((columns, RING * RING * rows), jnp.bfloat16),
            VMEM((columns, RING * RING * rows), jnp.bfloat16),
            VMEM((8, LANES), jnp.float32),
            VMEM((8, LANES), jnp.float32),
            VMEM((16 * strips, LANES), jnp.bfloat16),
            VMEM((columns, rows), jnp.float32),
            VMEM((columns, rows), jnp.float32),
        ],
        in_specs=[pl.BlockSpec(memory_space=pltpu.HBM)] * 6 + [space],
        out_specs=[space] * 7,
        scratch_shapes=[
            VMEM((6, columns, rows), jnp.float32),
            VMEM((RING * RING, 16, LANES), jnp.float32),
            VMEM((n_width, 16, LANES), jnp.float32),
            VMEM((16 * strips, LANES), jnp.float32),
            DMA((6,)),
            DMA((RING * RING - 1,)),
            DMA((RING * RING - 1,)),
            DMA((n_width - 1,)),
            DMA((n_width - 1,)),
            DMA((n_copies,)),
            DMA((n_copies,)),
        ],
        compiler_params=pltpu.CompilerParams(collective_id=0, has_side_effects=True, vmem_limit_bytes=32 * 2**20),
    )(*(pltpu.with_memory_space_constraint(a.T, pltpu.HBM)
        for a in (train_gate, drift_gate, spread_gate, train_up, drift_up, spread_up)), norm)
    return (
        og.T, ou.T, scale_g.reshape(-1)[:columns], scale_u.reshape(-1)[:columns],
        serve.reshape(-1), wg.T, wu.T,
    )


def solution(mesh):
    split = Mesh(mesh.devices.reshape(RING, RING, mesh.shape["width"]), FSDP_WIDTH)
    weights = P(FSDP, "width")
    return jax.shard_map(
        functools.partial(shards, mesh.shape["width"]),
        mesh=split,
        in_specs=(weights,) * 6 + (P(FSDP_WIDTH),) * 2,
        out_specs=(P(None, "width"), P(None, "width"), P("width"), P("width"), P(), weights, weights),
        check_vma=False,
    )
```

```python
import functools

import jax
import jax.numpy as jnp
from jax import lax
from jax.experimental import pallas as pl
from jax.experimental.pallas import tpu as pltpu
from jax.sharding import Mesh
from jax.sharding import PartitionSpec as P

FSDP = ("fsdp_0", "fsdp_1")
FSDP_WIDTH = ("fsdp_0", "fsdp_1", "width")
RING = 4
LANES = 128
NORM_ROW = 14

learn_rate = 0.3
hold_rate = 0.9


def chunks(columns):
    return [(at, min(LANES, columns - at)) for at in range(0, columns, LANES)]


def kernel(n_width, tg, dg, sg, tu, du, su, norm_old, norm_new,
           og, ou, scale_g, scale_u, serve, wg, wu,
           held, norms, sums, parts, ordered,
           in_sems, norm_sems, sum_send, sum_recv, part_send, part_recv, serve_send, serve_recv,
           send_sems, recv_sems, ready):
    y, x, w = lax.axis_index("fsdp_0"), lax.axis_index("fsdp_1"), lax.axis_index("width")
    me = y * RING + x
    columns, rows = wg.shape

    def at(yy, xx, ww):
        return {"device_id": (yy, xx, ww), "device_id_type": pl.DeviceIdType.MESH}

    norm_loads = [pltpu.make_async_copy(ref, norms.at[i], norm_sems.at[i])
                  for i, ref in enumerate((norm_old, norm_new))]
    loads = [pltpu.make_async_copy(ref, held.at[i], in_sems.at[i])
             for i, ref in enumerate((tg, dg, sg, tu, du, su))]
    for load in loads + norm_loads:
        load.start()

    plane = sorted(((dy, dx) for dy in range(RING) for dx in range(RING) if dy or dx),
                   key=lambda d: -(min(d[0], RING - d[0]) + min(d[1], RING - d[1])))
    mates = [((y + dy) % RING, (x + dx) % RING, w) for dy, dx in plane]
    stack = [(y, x, (w + dw) % n_width) for dw in range(1, n_width)]

    gateway, herald = me == 0, me == 1
    barrier = pltpu.get_barrier_semaphore()
    for peer in mates:
        @pl.when(peer[0] * RING + peer[1] != 0)
        def _():
            pl.semaphore_signal(barrier, 1, **at(*peer))

    @pl.when(gateway)
    def _():
        for peer in stack:
            pl.semaphore_signal(barrier, 1, **at(*peer))

    sums[me] = jnp.zeros((16, LANES), jnp.float32)
    for load in norm_loads:
        load.wait()
    gain = norms[0] + norms[1]
    length = gain.shape[1]
    lane = lax.broadcasted_iota(jnp.int32, (1, LANES), 1)
    spread = jnp.zeros((1, LANES), jnp.float32)
    for i in range(length):
        spread = jnp.where(lane == w * length % LANES + i, gain[:, i:i + 1], spread)
    sums[me, NORM_ROW:NORM_ROW + 1, :] = spread
    for a, whole in enumerate((wg, wu)):
        for load in loads[3 * a:3 * a + 3]:
            load.wait()
        for k, (start, size) in enumerate(chunks(columns)):
            part = pl.ds(start, size)
            hold = hold_rate * held[3 * a + 1, part, :] + held[3 * a + 2, part, :]
            new = held[3 * a, part, :] - learn_rate * hold
            whole[part, :] = new
            square = new * new
            folded = square[:, :LANES]
            for j in range(LANES, rows, LANES):
                folded = folded + square[:, j:j + LANES]
            if size < LANES:
                folded = jnp.concatenate([folded, jnp.zeros((LANES - size, LANES), jnp.float32)], axis=0)
            sums[me, 8 * a + k:8 * a + k + 1, :] = jnp.sum(folded.T, axis=0, keepdims=True)

    @pl.when(jnp.logical_not(gateway))
    def _():
        pl.semaphore_wait(barrier, len(mates))

    @pl.when(herald)
    def _():
        pl.semaphore_signal(ready, 1, **at(0, 0, w))

    @pl.when(gateway)
    def _():
        pl.semaphore_wait(ready, 1)

    sent = []
    for i, peer in enumerate(mates):
        copy = pltpu.make_async_remote_copy(sums.at[me], sums.at[me], sum_send.at[i], sum_recv.at[i], **at(*peer))
        copy.start()
        sent.append(copy)
    for i, (dy, dx) in enumerate(plane):
        source = ((y + RING - dy) % RING) * RING + (x + RING - dx) % RING
        pltpu.make_async_remote_copy(sums.at[source], sums.at[source], sum_send.at[i], sum_recv.at[i],
                                     **at(*mates[i])).wait_recv()
    total = sums[0]
    for i in range(1, RING * RING):
        total = total + sums[i]
    scale = jnp.sqrt(total)
    inverse = jnp.concatenate([1.0 / scale, jnp.zeros((LANES - 16, LANES), jnp.float32)], axis=0).T
    own = pl.ds(pl.multiple_of(me * rows, LANES), rows)
    for a, (whole, out) in enumerate(((wg, og), (wu, ou))):
        for k, (start, size) in enumerate(chunks(columns)):
            part = pl.ds(start, size)
            factor = inverse[:size, 8 * a + k:8 * a + k + 1]
            out[part, own] = (whole[part, :] * factor).astype(jnp.bfloat16)
    scale_g[...] = scale[:8]
    scale_u[...] = scale[8:]

    @pl.when(gateway)
    def _():
        for i in range(RING * RING):
            parts[w, i:i + 1, :] = sums[i, NORM_ROW:NORM_ROW + 1, :]

    half = columns // 2 // 8 * 8
    halves = {1: pl.ds(0, half), -1: pl.ds(half, columns - half)}
    full = pl.ds(0, columns)
    outs = (og, ou)
    keys = {}

    def block(a, p, q):
        p, q = (p + RING) % RING, (q + RING) % RING
        index = q * RING + p if a == 0 else p * RING + q
        return pl.ds(pl.multiple_of(index * rows, LANES), rows)

    def peer(a, phase, d):
        along_x = (a == 0) == (phase == 1)
        if along_x:
            return at(y, (x + d + RING) % RING, w)
        return at((y + d + RING) % RING, x, w)

    def copy_of(key, a, phase, d, part, cols):
        index = keys.setdefault(key, len(keys))
        ref = outs[a].at[part, cols]
        return pltpu.make_async_remote_copy(ref, ref, send_sems.at[index], recv_sems.at[index], **peer(a, phase, d))

    def send(key, a, phase, d, part, cols):
        copy = copy_of(key, a, phase, d, part, cols)
        copy.start()
        sent.append(copy)

    def receive(key, a, phase, d, part, cols):
        copy_of(key, a, phase, d, part, cols).wait_recv()

    spots = ((x, y), (y, x))
    both = [(a, d) for a in range(2) for d in (1, -1)]
    for a, d in both:
        p, q = spots[a]
        send(("first", a, d), a, 1, d, full, block(a, p, q))
    for a, d in both:
        p, q = spots[a]
        send(("second", a, 0, d), a, 2, d, full, block(a, p, q))
    for a, d in both:
        p, q = spots[a]
        receive(("first", a, d), a, 1, d, full, block(a, p - d, q))
        send(("pass", a, d), a, 1, d, halves[d], block(a, p - d, q))
    for a, e in both:
        p, q = spots[a]
        for d in (1, -1):
            send(("second", a, e, d), a, 2, d, full, block(a, p - e, q))
    for a, e in both:
        p, q = spots[a]
        receive(("pass", a, e), a, 1, e, halves[e], block(a, p - 2 * e, q))
        for d in (1, -1):
            send(("second", a, 2 * e, d), a, 2, d, halves[e], block(a, p + 2, q))

    def part_copy(i, slot):
        return pltpu.make_async_remote_copy(parts.at[slot], parts.at[slot], part_send.at[i], part_recv.at[i],
                                            **at(*stack[i]))

    def serve_copy(i, peer):
        return pltpu.make_async_remote_copy(serve, serve, serve_send.at[i], serve_recv, **at(*peer))

    @pl.when(gateway)
    def _():
        pl.semaphore_wait(barrier, len(stack))
        for i in range(len(stack)):
            part_copy(i, w).start()
        for i in range(len(stack)):
            part_copy(i, (w + n_width - (i + 1)) % n_width).wait_recv()
        strips = ordered.shape[0] // 16
        for b in range(strips):
            group = [parts[i] for i in range(b * n_width // strips, (b + 1) * n_width // strips)]
            ordered[pl.ds(b, 16, stride=strips), :] = functools.reduce(jnp.add, group)
        serve[...] = ordered[...].astype(jnp.bfloat16)
        for i in range(len(stack)):
            part_copy(i, w).wait_send()
        for i, peer in enumerate(mates):
            serve_copy(i, peer).start()

    for e in (0, 1, -1):
        for a, d in both:
            p, q = spots[a]
            receive(("second", a, e, d), a, 2, d, full, block(a, p - e, q - d))
            send(("end", a, e, d), a, 2, d, halves[d], block(a, p - e, q - d))
    for a, d in both:
        p, q = spots[a]
        receive(("second", a, 2 * d, d), a, 2, d, halves[d], block(a, p + 2, q - d))
        send(("end", a, 2, d), a, 2, d, halves[d], block(a, p + 2, q - d))

    for a, d in both:
        p, q = spots[a]
        receive(("second", a, -2 * d, d), a, 2, d, halves[-d], block(a, p + 2, q - d))
    for e in (0, 1, -1, 2):
        for a, d in both:
            p, q = spots[a]
            receive(("end", a, e, d), a, 2, d, halves[d], block(a, p - e, q - 2 * d))
    for copy in sent:
        copy.wait_send()

    @pl.when(gateway)
    def _():
        for i, peer in enumerate(mates):
            serve_copy(i, peer).wait_send()

    @pl.when(jnp.logical_not(gateway))
    def _():
        serve_copy(0, mates[0]).wait_recv()


def flush(*refs):
    n = len(refs) // 2
    sources, targets, sems = refs[:n], refs[n:2 * n], refs[2 * n]
    copies = []
    for source, target in zip(sources, targets):
        rows = source.shape[0]
        pieces = 4 if rows >= LANES else 1
        size = -(-rows // pieces // 16) * 16
        for start in range(0, rows, size):
            part = pl.ds(start, min(size, rows - start))
            copies.append(pltpu.make_async_copy(source.at[part], target.at[part], sems.at[len(copies)]))
    for copy in copies:
        copy.start()
    for copy in copies:
        copy.wait()


def shards(n_width, train_gate, drift_gate, spread_gate, train_up, drift_up, spread_up, norm_train, norm_step):
    rows, columns = train_gate.shape
    length = norm_train.shape[0]
    strips = n_width * length // LANES
    n_copies = 2 * 22
    VMEM, DMA = pltpu.VMEM, pltpu.SemaphoreType.DMA
    space = pl.BlockSpec(memory_space=pltpu.VMEM)
    on_chip = pl.pallas_call(
        functools.partial(kernel, n_width),
        out_shape=[
            VMEM((columns, RING * RING * rows), jnp.bfloat16),
            VMEM((columns, RING * RING * rows), jnp.bfloat16),
            VMEM((8, LANES), jnp.float32),
            VMEM((8, LANES), jnp.float32),
            VMEM((16 * strips, LANES), jnp.bfloat16),
            VMEM((columns, rows), jnp.float32),
            VMEM((columns, rows), jnp.float32),
        ],
        in_specs=[pl.BlockSpec(memory_space=pltpu.HBM)] * 8,
        out_specs=[space] * 7,
        scratch_shapes=[
            VMEM((6, columns, rows), jnp.float32),
            VMEM((2, 1, length), jnp.float32),
            VMEM((RING * RING, 16, LANES), jnp.float32),
            VMEM((n_width, 16, LANES), jnp.float32),
            VMEM((16 * strips, LANES), jnp.float32),
            DMA((6,)),
            DMA((2,)),
            DMA((RING * RING - 1,)),
            DMA((RING * RING - 1,)),
            DMA((n_width - 1,)),
            DMA((n_width - 1,)),
            DMA((RING * RING - 1,)),
            DMA(()),
            DMA((n_copies,)),
            DMA((n_copies,)),
            pltpu.SemaphoreType.REGULAR,
        ],
        compiler_params=pltpu.CompilerParams(collective_id=0, has_side_effects=True, vmem_limit_bytes=32 * 2**20),
    )(*(pltpu.with_memory_space_constraint(a, pltpu.HBM) for a in (
        train_gate.T, drift_gate.T, spread_gate.T, train_up.T, drift_up.T, spread_up.T,
        norm_train.reshape(1, length), norm_step.reshape(1, length))))
    og, ou, scale_g, scale_u, serve, wg, wu = pl.pallas_call(
        flush,
        out_shape=[pltpu.HBM(a.shape, a.dtype) for a in on_chip],
        in_specs=[space] * 7,
        out_specs=[pl.BlockSpec(memory_space=pltpu.HBM)] * 7,
        scratch_shapes=[DMA((19,))],
        compiler_params=pltpu.CompilerParams(vmem_limit_bytes=2**20),
    )(*(pltpu.with_memory_space_constraint(a, pltpu.VMEM) for a in on_chip))
    return (
        og.T, ou.T, scale_g.reshape(-1)[:columns], scale_u.reshape(-1)[:columns],
        serve.reshape(-1), wg.T, wu.T,
    )


def solution(mesh):
    split = Mesh(mesh.devices.reshape(RING, RING, mesh.shape["width"]), FSDP_WIDTH)
    weights = P(FSDP, "width")
    return jax.shard_map(
        functools.partial(shards, mesh.shape["width"]),
        mesh=split,
        in_specs=(weights,) * 6 + (P(FSDP_WIDTH),) * 2,
        out_specs=(P(None, "width"), P(None, "width"), P("width"), P("width"), P(), weights, weights),
        check_vma=False,
    )
```

```python
import functools

import jax
import jax.numpy as jnp
from jax import lax
from jax.experimental import pallas as pl
from jax.experimental.pallas import tpu as pltpu
from jax.sharding import Mesh
from jax.sharding import PartitionSpec as P

FSDP = ("fsdp_0", "fsdp_1")
FSDP_WIDTH = ("fsdp_0", "fsdp_1", "width")
RING = 4
LANES = 128
NORM_ROW = 14
EARLY = 112

learn_rate = 0.3
hold_rate = 0.9


def chunks(columns):
    return [(at, min(LANES, columns - at)) for at in range(0, columns, LANES)]


def kernel(n_width, early, tg, dg, sg, tu, du, su, norm_old, norm_new,
           og, ou, scale_g, scale_u, serve, wg, wu,
           held, raw, norms, sums, parts, ordered,
           in_sems, norm_sems, sum_send, sum_recv, part_send, part_recv, serve_send, serve_recv,
           send_sems, recv_sems, ready):
    y, x, w = lax.axis_index("fsdp_0"), lax.axis_index("fsdp_1"), lax.axis_index("width")
    me = y * RING + x
    columns, rows = wg.shape

    def at(yy, xx, ww):
        return {"device_id": (yy, xx, ww), "device_id_type": pl.DeviceIdType.MESH}

    norm_loads = [pltpu.make_async_copy(ref, norms.at[i], norm_sems.at[i])
                  for i, ref in enumerate((norm_old, norm_new))]
    loads = [pltpu.make_async_copy(ref, held.at[i], in_sems.at[i])
             for i, ref in enumerate((tg, dg, sg, tu, du, su))]
    for load in loads + norm_loads:
        load.start()

    plane = sorted(((dy, dx) for dy in range(RING) for dx in range(RING) if dy or dx),
                   key=lambda d: -(min(d[0], RING - d[0]) + min(d[1], RING - d[1])))
    mates = [((y + dy) % RING, (x + dx) % RING, w) for dy, dx in plane]
    stack = [(y, x, (w + dw) % n_width) for dw in range(1, n_width)]

    gateway, herald = me == 0, me == 1
    barrier = pltpu.get_barrier_semaphore()
    for peer in mates:
        @pl.when(peer[0] * RING + peer[1] != 0)
        def _():
            pl.semaphore_signal(barrier, 1, **at(*peer))

    @pl.when(gateway)
    def _():
        for peer in stack:
            pl.semaphore_signal(barrier, 1, **at(*peer))

    sums[me] = jnp.zeros((16, LANES), jnp.float32)
    for load in norm_loads:
        load.wait()
    gain = norms[0] + norms[1]
    length = gain.shape[1]
    lane = lax.broadcasted_iota(jnp.int32, (1, LANES), 1)
    spread = jnp.zeros((1, LANES), jnp.float32)
    for i in range(length):
        spread = jnp.where(lane == w * length % LANES + i, gain[:, i:i + 1], spread)
    sums[me, NORM_ROW:NORM_ROW + 1, :] = spread
    for a, whole in enumerate((wg, wu)):
        for load in loads[3 * a:3 * a + 3]:
            load.wait()
        for k, (start, size) in enumerate(chunks(columns)):
            part = pl.ds(start, size)
            hold = hold_rate * held[3 * a + 1, part, :] + held[3 * a + 2, part, :]
            new = held[3 * a, part, :] - learn_rate * hold
            whole[part, :] = new
            square = new * new
            folded = square[:, :LANES]
            for j in range(LANES, rows, LANES):
                folded = folded + square[:, j:j + LANES]
            if size < LANES:
                folded = jnp.concatenate([folded, jnp.zeros((LANES - size, LANES), jnp.float32)], axis=0)
            sums[me, 8 * a + k:8 * a + k + 1, :] = jnp.sum(folded.T, axis=0, keepdims=True)

    @pl.when(jnp.logical_not(gateway))
    def _():
        pl.semaphore_wait(barrier, len(mates))

    @pl.when(herald)
    def _():
        pl.semaphore_signal(ready, 1, **at(0, 0, w))

    @pl.when(gateway)
    def _():
        pl.semaphore_wait(ready, 1)

    half = columns // 2 // 8 * 8
    halves = {1: pl.ds(0, half), -1: pl.ds(half, columns - half)}
    full, late = pl.ds(0, columns), pl.ds(early, columns - early)
    outs = (og, ou)
    keys = {}

    def block(a, p, q):
        p, q = (p + RING) % RING, (q + RING) % RING
        index = q * RING + p if a == 0 else p * RING + q
        return pl.ds(pl.multiple_of(index * rows, LANES), rows)

    def peer(a, phase, d):
        along_x = (a == 0) == (phase == 1)
        if along_x:
            return at(y, (x + d + RING) % RING, w)
        return at((y + d + RING) % RING, x, w)

    def copy_of(key, a, phase, d, part, cols):
        index = keys.setdefault(key, len(keys))
        ref = outs[a].at[part, cols]
        return pltpu.make_async_remote_copy(ref, ref, send_sems.at[index], recv_sems.at[index], **peer(a, phase, d))

    def send(key, a, phase, d, part, cols):
        copy = copy_of(key, a, phase, d, part, cols)
        copy.start()
        sent.append(copy)

    def receive(key, a, phase, d, part, cols):
        copy_of(key, a, phase, d, part, cols).wait_recv()

    spots = ((x, y), (y, x))
    both = [(a, d) for a in range(2) for d in (1, -1)]
    sent = []
    for i, mate in enumerate(mates):
        copy = pltpu.make_async_remote_copy(sums.at[me], sums.at[me], sum_send.at[i], sum_recv.at[i], **at(*mate))
        copy.start()
        sent.append(copy)

    def raw_copy(a, d):
        index = keys.setdefault(("raw", a, d), len(keys))
        return pltpu.make_async_remote_copy((wg, wu)[a].at[pl.ds(0, early)], raw.at[a, (1 - d) // 2],
                                            send_sems.at[index], recv_sems.at[index], **peer(a, 1, d))

    for a, d in both:
        copy = raw_copy(a, d)
        copy.start()
        sent.append(copy)
    for i, (dy, dx) in enumerate(plane):
        source = ((y + RING - dy) % RING) * RING + (x + RING - dx) % RING
        pltpu.make_async_remote_copy(sums.at[source], sums.at[source], sum_send.at[i], sum_recv.at[i],
                                     **at(*mates[i])).wait_recv()
    total = sums[0]
    for i in range(1, RING * RING):
        total = total + sums[i]
    scale = jnp.sqrt(total)
    inverse = jnp.concatenate([1.0 / scale, jnp.zeros((LANES - 16, LANES), jnp.float32)], axis=0).T

    def scaled(a, source, count, cols):
        for k, (start, size) in enumerate(chunks(count)):
            part = pl.ds(start, size)
            factor = inverse[:size, 8 * a + k:8 * a + k + 1]
            outs[a][part, cols] = (source[part, :] * factor).astype(jnp.bfloat16)

    for a, whole in enumerate((wg, wu)):
        scaled(a, whole, columns, pl.ds(pl.multiple_of(me * rows, LANES), rows))
    scale_g[...] = scale[:8]
    scale_u[...] = scale[8:]

    @pl.when(gateway)
    def _():
        for i in range(RING * RING):
            parts[w, i:i + 1, :] = sums[i, NORM_ROW:NORM_ROW + 1, :]

    for a, d in both:
        p, q = spots[a]
        send(("first", a, d), a, 1, d, late, block(a, p, q))
    for a, d in both:
        p, q = spots[a]
        send(("second", a, 0, d), a, 2, d, full, block(a, p, q))
    for a, d in both:
        p, q = spots[a]
        raw_copy(a, d).wait_recv()
        scaled(a, raw.at[a, (1 - d) // 2], early, block(a, p - d, q))
    for a, d in both:
        p, q = spots[a]
        receive(("first", a, d), a, 1, d, late, block(a, p - d, q))
        send(("pass", a, d), a, 1, d, halves[d], block(a, p - d, q))
    for a, e in both:
        p, q = spots[a]
        for d in (1, -1):
            send(("second", a, e, d), a, 2, d, full, block(a, p - e, q))
    for a, e in both:
        p, q = spots[a]
        receive(("pass", a, e), a, 1, e, halves[e], block(a, p - 2 * e, q))
        for d in (1, -1):
            send(("second", a, 2 * e, d), a, 2, d, halves[e], block(a, p + 2, q))

    def part_copy(i, slot):
        return pltpu.make_async_remote_copy(parts.at[slot], parts.at[slot], part_send.at[i], part_recv.at[i],
                                            **at(*stack[i]))

    def serve_copy(i, peer):
        return pltpu.make_async_remote_copy(serve, serve, serve_send.at[i], serve_recv, **at(*peer))

    @pl.when(gateway)
    def _():
        pl.semaphore_wait(barrier, len(stack))
        for i in range(len(stack)):
            part_copy(i, w).start()
        for i in range(len(stack)):
            part_copy(i, (w + n_width - (i + 1)) % n_width).wait_recv()
        strips = ordered.shape[0] // 16
        for b in range(strips):
            group = [parts[i] for i in range(b * n_width // strips, (b + 1) * n_width // strips)]
            ordered[pl.ds(b, 16, stride=strips), :] = functools.reduce(jnp.add, group)
        serve[...] = ordered[...].astype(jnp.bfloat16)
        for i in range(len(stack)):
            part_copy(i, w).wait_send()
        for i, peer in enumerate(mates):
            serve_copy(i, peer).start()

    for e in (0, 1, -1):
        for a, d in both:
            p, q = spots[a]
            receive(("second", a, e, d), a, 2, d, full, block(a, p - e, q - d))
            send(("end", a, e, d), a, 2, d, halves[d], block(a, p - e, q - d))
    for a, d in both:
        p, q = spots[a]
        receive(("second", a, 2 * d, d), a, 2, d, halves[d], block(a, p + 2, q - d))
        send(("end", a, 2, d), a, 2, d, halves[d], block(a, p + 2, q - d))

    for a, d in both:
        p, q = spots[a]
        receive(("second", a, -2 * d, d), a, 2, d, halves[-d], block(a, p + 2, q - d))
    for e in (0, 1, -1, 2):
        for a, d in both:
            p, q = spots[a]
            receive(("end", a, e, d), a, 2, d, halves[d], block(a, p - e, q - 2 * d))
    for copy in sent:
        copy.wait_send()

    @pl.when(gateway)
    def _():
        for i, peer in enumerate(mates):
            serve_copy(i, peer).wait_send()

    @pl.when(jnp.logical_not(gateway))
    def _():
        serve_copy(0, mates[0]).wait_recv()


def flush(*refs):
    n = len(refs) // 2
    sources, targets, sems = refs[:n], refs[n:2 * n], refs[2 * n]
    copies = []
    for source, target in zip(sources, targets):
        rows = source.shape[0]
        pieces = 4 if rows >= LANES else 1
        size = -(-rows // pieces // 16) * 16
        for start in range(0, rows, size):
            part = pl.ds(start, min(size, rows - start))
            copies.append(pltpu.make_async_copy(source.at[part], target.at[part], sems.at[len(copies)]))
    for copy in copies:
        copy.start()
    for copy in copies:
        copy.wait()


def shards(n_width, train_gate, drift_gate, spread_gate, train_up, drift_up, spread_up, norm_train, norm_step):
    rows, columns = train_gate.shape
    length = norm_train.shape[0]
    strips = n_width * length // LANES
    n_copies = 2 * 24
    early = min(EARLY, columns // 16 * 8)
    VMEM, DMA = pltpu.VMEM, pltpu.SemaphoreType.DMA
    space = pl.BlockSpec(memory_space=pltpu.VMEM)
    on_chip = pl.pallas_call(
        functools.partial(kernel, n_width, early),
        out_shape=[
            VMEM((columns, RING * RING * rows), jnp.bfloat16),
            VMEM((columns, RING * RING * rows), jnp.bfloat16),
            VMEM((8, LANES), jnp.float32),
            VMEM((8, LANES), jnp.float32),
            VMEM((16 * strips, LANES), jnp.bfloat16),
            VMEM((columns, rows), jnp.float32),
            VMEM((columns, rows), jnp.float32),
        ],
        in_specs=[pl.BlockSpec(memory_space=pltpu.HBM)] * 8,
        out_specs=[space] * 7,
        scratch_shapes=[
            VMEM((6, columns, rows), jnp.float32),
            VMEM((2, 2, early, rows), jnp.float32),
            VMEM((2, 1, length), jnp.float32),
            VMEM((RING * RING, 16, LANES), jnp.float32),
            VMEM((n_width, 16, LANES), jnp.float32),
            VMEM((16 * strips, LANES), jnp.float32),
            DMA((6,)),
            DMA((2,)),
            DMA((RING * RING - 1,)),
            DMA((RING * RING - 1,)),
            DMA((n_width - 1,)),
            DMA((n_width - 1,)),
            DMA((RING * RING - 1,)),
            DMA(()),
            DMA((n_copies,)),
            DMA((n_copies,)),
            pltpu.SemaphoreType.REGULAR,
        ],
        compiler_params=pltpu.CompilerParams(collective_id=0, has_side_effects=True, vmem_limit_bytes=32 * 2**20),
    )(*(pltpu.with_memory_space_constraint(a, pltpu.HBM) for a in (
        train_gate.T, drift_gate.T, spread_gate.T, train_up.T, drift_up.T, spread_up.T,
        norm_train.reshape(1, length), norm_step.reshape(1, length))))
    og, ou, scale_g, scale_u, serve, wg, wu = pl.pallas_call(
        flush,
        out_shape=[pltpu.HBM(a.shape, a.dtype) for a in on_chip],
        in_specs=[space] * 7,
        out_specs=[pl.BlockSpec(memory_space=pltpu.HBM)] * 7,
        scratch_shapes=[DMA((19,))],
        compiler_params=pltpu.CompilerParams(vmem_limit_bytes=2**20),
    )(*(pltpu.with_memory_space_constraint(a, pltpu.VMEM) for a in on_chip))
    return (
        og.T, ou.T, scale_g.reshape(-1)[:columns], scale_u.reshape(-1)[:columns],
        serve.reshape(-1), wg.T, wu.T,
    )


def solution(mesh):
    split = Mesh(mesh.devices.reshape(RING, RING, mesh.shape["width"]), FSDP_WIDTH)
    weights = P(FSDP, "width")
    return jax.shard_map(
        functools.partial(shards, mesh.shape["width"]),
        mesh=split,
        in_specs=(weights,) * 6 + (P(FSDP_WIDTH),) * 2,
        out_specs=(P(None, "width"), P(None, "width"), P("width"), P("width"), P(), weights, weights),
        check_vma=False,
    )
```

```python
import functools

import jax
import jax.numpy as jnp
from jax import lax
from jax.experimental import pallas as pl
from jax.experimental.pallas import tpu as pltpu
from jax.sharding import Mesh
from jax.sharding import PartitionSpec as P

FSDP = ("fsdp_0", "fsdp_1")
FSDP_WIDTH = ("fsdp_0", "fsdp_1", "width")
RING = 4
LANES = 128
HALF_ROWS = 6
EARLY = 128

learn_rate = 0.3
hold_rate = 0.9


def chunks(columns):
    return [(at, min(LANES, columns - at)) for at in range(0, columns, LANES)]


def kernel(n_width, early, tg, dg, sg, tu, du, su, norm_old, norm_new,
           og, ou, scale_g, scale_u, serve, wg, wu,
           held, raw, norms, sums, parts, ordered,
           in_sems, norm_sems, sum_send, sum_recv, part_send, part_recv, serve_send, serve_recv,
           send_sems, recv_sems, ready):
    y, x, w = lax.axis_index("fsdp_0"), lax.axis_index("fsdp_1"), lax.axis_index("width")
    me = y * RING + x
    columns, rows = wg.shape

    def at(yy, xx, ww):
        return {"device_id": (yy, xx, ww), "device_id_type": pl.DeviceIdType.MESH}

    norm_loads = [pltpu.make_async_copy(ref, norms.at[i], norm_sems.at[i])
                  for i, ref in enumerate((norm_old, norm_new))]
    loads = [pltpu.make_async_copy(ref, held.at[i], in_sems.at[i])
             for i, ref in enumerate((tg, dg, sg, tu, du, su))]
    for load in loads + norm_loads:
        load.start()

    plane = sorted(((dy, dx) for dy in range(RING) for dx in range(RING) if dy or dx),
                   key=lambda d: -(min(d[0], RING - d[0]) + min(d[1], RING - d[1])))
    mates = [((y + dy) % RING, (x + dx) % RING, w) for dy, dx in plane]
    stack = [(y, x, (w + dw) % n_width) for dw in range(1, n_width)]

    gateway, herald = me == 0, me == 1
    barrier = pltpu.get_barrier_semaphore()
    for peer in mates:
        @pl.when(peer[0] * RING + peer[1] != 0)
        def _():
            pl.semaphore_signal(barrier, 1, **at(*peer))

    @pl.when(gateway)
    def _():
        for peer in stack:
            pl.semaphore_signal(barrier, 1, **at(*peer))

    sums[me] = jnp.zeros((2 * HALF_ROWS, LANES), jnp.float32)
    for load in norm_loads:
        load.wait()
    gain = norms[0] + norms[1]
    length = gain.shape[1]
    lane = lax.broadcasted_iota(jnp.int32, (1, LANES), 1)
    spread = jnp.zeros((1, LANES), jnp.float32)
    for i in range(length):
        spread = jnp.where(lane == LANES - length + i, gain[:, i:i + 1], spread)
    sums[me, HALF_ROWS - 1:HALF_ROWS, :] = spread
    for a, whole in enumerate((wg, wu)):
        for load in loads[3 * a:3 * a + 3]:
            load.wait()
        for k, (start, size) in enumerate(chunks(columns)):
            part = pl.ds(start, size)
            hold = hold_rate * held[3 * a + 1, part, :] + held[3 * a + 2, part, :]
            new = held[3 * a, part, :] - learn_rate * hold
            whole[part, :] = new
            square = new * new
            folded = square[:, :LANES]
            for j in range(LANES, rows, LANES):
                folded = folded + square[:, j:j + LANES]
            if size < LANES:
                folded = jnp.concatenate([folded, jnp.zeros((LANES - size, LANES), jnp.float32)], axis=0)
            line = jnp.sum(folded.T, axis=0, keepdims=True)
            row = HALF_ROWS * a + k
            sums[me, row:row + 1, :] = line + spread if row == HALF_ROWS - 1 else line

    @pl.when(jnp.logical_not(gateway))
    def _():
        pl.semaphore_wait(barrier, len(mates))

    @pl.when(herald)
    def _():
        pl.semaphore_signal(ready, 1, **at(0, 0, w))

    @pl.when(gateway)
    def _():
        pl.semaphore_wait(ready, 1)

    half = columns // 2 // 8 * 8
    halves = {1: pl.ds(0, half), -1: pl.ds(half, columns - half)}
    full, late = pl.ds(0, columns), pl.ds(early, columns - early)
    outs = (og, ou)
    keys = {}

    def block(a, p, q):
        p, q = (p + RING) % RING, (q + RING) % RING
        index = q * RING + p if a == 0 else p * RING + q
        return pl.ds(pl.multiple_of(index * rows, LANES), rows)

    def peer(a, phase, d):
        along_x = (a == 0) == (phase == 1)
        if along_x:
            return at(y, (x + d + RING) % RING, w)
        return at((y + d + RING) % RING, x, w)

    def copy_of(key, a, phase, d, part, cols):
        index = keys.setdefault(key, len(keys))
        ref = outs[a].at[part, cols]
        return pltpu.make_async_remote_copy(ref, ref, send_sems.at[index], recv_sems.at[index], **peer(a, phase, d))

    def send(key, a, phase, d, part, cols):
        copy = copy_of(key, a, phase, d, part, cols)
        copy.start()
        sent.append(copy)

    def receive(key, a, phase, d, part, cols):
        copy_of(key, a, phase, d, part, cols).wait_recv()

    spots = ((x, y), (y, x))
    both = [(a, d) for a in range(2) for d in (1, -1)]
    sent = []
    for i, mate in enumerate(mates):
        copy = pltpu.make_async_remote_copy(sums.at[me], sums.at[me], sum_send.at[i], sum_recv.at[i], **at(*mate))
        copy.start()
        sent.append(copy)

    def raw_copy(a, d):
        index = keys.setdefault(("raw", a, d), len(keys))
        return pltpu.make_async_remote_copy((wg, wu)[a].at[pl.ds(0, early)], raw.at[a, (1 - d) // 2],
                                            send_sems.at[index], recv_sems.at[index], **peer(a, 1, d))

    for a, d in both:
        copy = raw_copy(a, d)
        copy.start()
        sent.append(copy)
    for i, (dy, dx) in enumerate(plane):
        source = ((y + RING - dy) % RING) * RING + (x + RING - dx) % RING
        pltpu.make_async_remote_copy(sums.at[source], sums.at[source], sum_send.at[i], sum_recv.at[i],
                                     **at(*mates[i])).wait_recv()
    total = sums[0]
    for i in range(1, RING * RING):
        total = total + sums[i]
    scale = jnp.sqrt(total)
    inverse = jnp.concatenate([1.0 / scale, jnp.zeros((LANES - 2 * HALF_ROWS, LANES), jnp.float32)], axis=0).T

    def scaled(a, source, count, cols):
        for k, (start, size) in enumerate(chunks(count)):
            part = pl.ds(start, size)
            factor = inverse[:size, HALF_ROWS * a + k:HALF_ROWS * a + k + 1]
            outs[a][part, cols] = (source[part, :] * factor).astype(jnp.bfloat16)

    for a, whole in enumerate((wg, wu)):
        scaled(a, whole, columns, pl.ds(pl.multiple_of(me * rows, LANES), rows))
    for a, out in enumerate((scale_g, scale_u)):
        out[...] = jnp.zeros_like(out)
        out[:HALF_ROWS, :] = scale[HALF_ROWS * a:HALF_ROWS * (a + 1)]

    @pl.when(gateway)
    def _():
        for i in range(RING * RING):
            parts[w, i:i + 1, :] = sums[i, HALF_ROWS - 1:HALF_ROWS, :]
        gains, placed = parts[w], jnp.zeros((16, LANES), jnp.float32)
        for i in range(length):
            placed = jnp.where(lane == w * length % LANES + i, gains[:, LANES - length + i:LANES - length + i + 1], placed)
        parts[w] = placed

    def land_raw():
        for a, d in both:
            p, q = spots[a]
            raw_copy(a, d).wait_recv()
            scaled(a, raw.at[a, (1 - d) // 2], early, block(a, p - d, q))

    first_core = w % 2 == 0
    pl.when(first_core)(land_raw)
    for a, d in both:
        p, q = spots[a]
        send(("first", a, d), a, 1, d, late, block(a, p, q))
    for a, d in both:
        p, q = spots[a]
        send(("second", a, 0, d), a, 2, d, full, block(a, p, q))
    pl.when(jnp.logical_not(first_core))(land_raw)
    for a, d in both:
        p, q = spots[a]
        receive(("first", a, d), a, 1, d, late, block(a, p - d, q))
        send(("pass", a, d), a, 1, d, halves[d], block(a, p - d, q))
    for a, e in both:
        p, q = spots[a]
        for d in (1, -1):
            send(("second", a, e, d), a, 2, d, full, block(a, p - e, q))
    for a, e in both:
        p, q = spots[a]
        receive(("pass", a, e), a, 1, e, halves[e], block(a, p - 2 * e, q))
        for d in (1, -1):
            send(("second", a, 2 * e, d), a, 2, d, halves[e], block(a, p + 2, q))

    def part_copy(i, slot):
        return pltpu.make_async_remote_copy(parts.at[slot], parts.at[slot], part_send.at[i], part_recv.at[i],
                                            **at(*stack[i]))

    def serve_copy(i, peer):
        return pltpu.make_async_remote_copy(serve, serve, serve_send.at[i], serve_recv, **at(*peer))

    @pl.when(gateway)
    def _():
        pl.semaphore_wait(barrier, len(stack))
        for i in range(len(stack)):
            part_copy(i, w).start()
        for i in range(len(stack)):
            part_copy(i, (w + n_width - (i + 1)) % n_width).wait_recv()
        strips = ordered.shape[0] // 16
        for b in range(strips):
            group = [parts[i] for i in range(b * n_width // strips, (b + 1) * n_width // strips)]
            ordered[pl.ds(b, 16, stride=strips), :] = functools.reduce(jnp.add, group)
        serve[...] = ordered[...].astype(jnp.bfloat16)
        for i in range(len(stack)):
            part_copy(i, w).wait_send()
        for i, peer in enumerate(mates):
            serve_copy(i, peer).start()

    for e in (0, 1, -1):
        for a, d in both:
            p, q = spots[a]
            receive(("second", a, e, d), a, 2, d, full, block(a, p - e, q - d))
            send(("end", a, e, d), a, 2, d, halves[d], block(a, p - e, q - d))
    for a, d in both:
        p, q = spots[a]
        receive(("second", a, 2 * d, d), a, 2, d, halves[d], block(a, p + 2, q - d))
        send(("end", a, 2, d), a, 2, d, halves[d], block(a, p + 2, q - d))

    for a, d in both:
        p, q = spots[a]
        receive(("second", a, -2 * d, d), a, 2, d, halves[-d], block(a, p + 2, q - d))
    for e in (0, 1, -1, 2):
        for a, d in both:
            p, q = spots[a]
            receive(("end", a, e, d), a, 2, d, halves[d], block(a, p - e, q - 2 * d))
    for copy in sent:
        copy.wait_send()

    @pl.when(gateway)
    def _():
        for i, peer in enumerate(mates):
            serve_copy(i, peer).wait_send()

    @pl.when(jnp.logical_not(gateway))
    def _():
        serve_copy(0, mates[0]).wait_recv()


def flush(*refs):
    n = len(refs) // 2
    sources, targets, sems = refs[:n], refs[n:2 * n], refs[2 * n]
    copies = []
    for source, target in zip(sources, targets):
        rows = source.shape[0]
        pieces = 4 if rows >= LANES else 1
        size = -(-rows // pieces // 16) * 16
        for start in range(0, rows, size):
            part = pl.ds(start, min(size, rows - start))
            copies.append(pltpu.make_async_copy(source.at[part], target.at[part], sems.at[len(copies)]))
    for copy in copies:
        copy.start()
    for copy in copies:
        copy.wait()


def shards(n_width, train_gate, drift_gate, spread_gate, train_up, drift_up, spread_up, norm_train, norm_step):
    rows, columns = train_gate.shape
    length = norm_train.shape[0]
    strips = n_width * length // LANES
    n_copies = 2 * 24
    early = min(EARLY, columns // 16 * 8)
    VMEM, DMA = pltpu.VMEM, pltpu.SemaphoreType.DMA
    space = pl.BlockSpec(memory_space=pltpu.VMEM)
    on_chip = pl.pallas_call(
        functools.partial(kernel, n_width, early),
        out_shape=[
            VMEM((columns, RING * RING * rows), jnp.bfloat16),
            VMEM((columns, RING * RING * rows), jnp.bfloat16),
            VMEM((8, LANES), jnp.float32),
            VMEM((8, LANES), jnp.float32),
            VMEM((16 * strips, LANES), jnp.bfloat16),
            VMEM((columns, rows), jnp.float32),
            VMEM((columns, rows), jnp.float32),
        ],
        in_specs=[pl.BlockSpec(memory_space=pltpu.HBM)] * 8,
        out_specs=[space] * 7,
        scratch_shapes=[
            VMEM((6, columns, rows), jnp.float32),
            VMEM((2, 2, early, rows), jnp.float32),
            VMEM((2, 1, length), jnp.float32),
            VMEM((RING * RING, 2 * HALF_ROWS, LANES), jnp.float32),
            VMEM((n_width, 16, LANES), jnp.float32),
            VMEM((16 * strips, LANES), jnp.float32),
            DMA((6,)),
            DMA((2,)),
            DMA((RING * RING - 1,)),
            DMA((RING * RING - 1,)),
            DMA((n_width - 1,)),
            DMA((n_width - 1,)),
            DMA((RING * RING - 1,)),
            DMA(()),
            DMA((n_copies,)),
            DMA((n_copies,)),
            pltpu.SemaphoreType.REGULAR,
        ],
        compiler_params=pltpu.CompilerParams(collective_id=0, has_side_effects=True, vmem_limit_bytes=32 * 2**20),
    )(*(pltpu.with_memory_space_constraint(a, pltpu.HBM) for a in (
        train_gate.T, drift_gate.T, spread_gate.T, train_up.T, drift_up.T, spread_up.T,
        norm_train.reshape(1, length), norm_step.reshape(1, length))))
    og, ou, scale_g, scale_u, serve, wg, wu = pl.pallas_call(
        flush,
        out_shape=[pltpu.HBM(a.shape, a.dtype) for a in on_chip],
        in_specs=[space] * 7,
        out_specs=[pl.BlockSpec(memory_space=pltpu.HBM)] * 7,
        scratch_shapes=[DMA((19,))],
        compiler_params=pltpu.CompilerParams(vmem_limit_bytes=2**20),
    )(*(pltpu.with_memory_space_constraint(a, pltpu.VMEM) for a in on_chip))
    return (
        og.T, ou.T, scale_g.reshape(-1)[:columns], scale_u.reshape(-1)[:columns],
        serve.reshape(-1), wg.T, wu.T,
    )


def solution(mesh):
    split = Mesh(mesh.devices.reshape(RING, RING, mesh.shape["width"]), FSDP_WIDTH)
    weights = P(FSDP, "width")
    return jax.shard_map(
        functools.partial(shards, mesh.shape["width"]),
        mesh=split,
        in_specs=(weights,) * 6 + (P(FSDP_WIDTH),) * 2,
        out_specs=(P(None, "width"), P(None, "width"), P("width"), P("width"), P(), weights, weights),
        check_vma=False,
    )
```
